128 devices in a mesh: scen: 32 (over z_hi, x, y), col: 4 (over z_lo, core).
Axes of the slice: x: 4, y: 4, z: 4 (z_hi: 2, z_lo: 2; z = z_hi * 2 + z_lo), core: 2. Of those that a mesh axis runs over, the one named last changes fastest.
Arguments:
- tech: bfloat16 [128, 2048, 4096], P('scen', None, 'col'), may hold values from -0.0234375 to 0.0234375
- recourse: bfloat16 [128, 2048, 1024], P('scen', None, 'col'), may hold values from -0.125 to 0.125
- rhs: float32 [32, 128, 2048], P(None, 'scen'), may hold values from -6 to 6
- cost_first: float32 [4096], P('col'), may hold values from -6 to 6
- cost_second: float32 [128, 1024], P('scen', 'col'), may hold values from -6 to 6
- cone_id: int32 [128, 2048], P('scen'), may hold values from 0 to 127, never falling along the last dimension, each value on 1 to 64 neighbouring positions
Outputs:
- first_section: float32 [32, 4096], P(None, 'col')
- second_section: float32 [32, 128, 1024], P(None, 'scen', 'col')
- slack: float32 [32, 128, 2048], P(None, 'scen', 'col')
- dual: float32 [32, 128, 2048], P(None, 'scen', 'col')
The draws below stay inside these ranges and needn't reach their ends.
Inputs may be any that keep to these rules, and one draw needn't show every extreme that they name: Along the rows of a scenario cone_id never falls; a cone holds 1 to 64 rows.
All inputs are finite; a program needn't handle non-finite values.
Results may differ from the reference program's by a relative error of at most 0.014.
Values may be sent and summed in bfloat16 or wider, within the bound.
A program may use at most 128 MiB of HBM per device.

```python
import math
import jax
import jax.numpy as jnp
import numpy as np
from jax import lax

M = 2048
NX = 4096
NY = 1024
NCONE = 128
CONE_MOST = 64
BATCH = 32
ITERS = 3
CG_STEPS = 3
SCENS = 128


def steps_of(key, shape, cuts, least, top_value):
    def one(dim, parts):
        draws = jax.random.uniform(jax.random.fold_in(jax.random.fold_in(key, 6), dim), (parts,), jnp.float32, least / len(cuts), top_value / len(cuts))
        return jnp.repeat(jnp.exp(draws), shape[dim] // parts).reshape((-1,) + (1,) * (len(shape) - dim - 1))

    gain = one(*cuts[0])
    for cut in cuts[1:]:
        gain = gain * one(*cut)
    return gain


def split_up(count, total, reach, slope):
    loads = [(1 << 20) // math.isqrt(grade ** slope) + 1 for grade in range(2, count + 1)]
    spare, holding = total - reach - (count - 1), [1] * (count - 1)
    while spare > 0:
        candidates = [i for i in range(count - 1) if holding[i] < reach]
        whole, left = sum([loads[i] for i in candidates]), spare
        for i in candidates:
            more = min(reach - holding[i], max(1, left * loads[i] // whole), spare)
            holding[i] = holding[i] + more
            spare = spare - more
    return np.array([reach] + holding)


def uneven_parts(rng, number_of, total, limit, lean):
    if number_of == 2:
        one = jax.random.randint(rng, (), max(1, total - limit), min(limit, total - 1) + 1)
        return jnp.stack([one, total - one])
    tallies = jnp.asarray(split_up(number_of, total, limit, lean), jnp.int32)
    couples = (number_of - 1) // 2
    source_of, receiver = tallies[1:1 + 2 * couples:2], tallies[2:2 + 2 * couples:2]
    room = jnp.minimum(source_of - 1, limit - receiver)
    moved = jax.random.randint(jax.random.fold_in(rng, 1), (couples,), 0, 1 << 20) % (room + 1)
    tallies = tallies.at[1:1 + 2 * couples:2].set(source_of - moved).at[2:2 + 2 * couples:2].set(receiver + moved)
    return tallies[jax.random.permutation(jax.random.fold_in(rng, 2), number_of)]


def bell_draw(key, shape, spread, reach, split=(), dtype=jnp.bfloat16):
    loudness = steps_of(key, shape, split, -0.22, 0.18) if split else 1.0
    entries = jax.random.normal(key, shape, jnp.float32) * spread * loudness
    return jnp.minimum(jnp.maximum(entries, -reach), reach).astype(dtype)


def setup_inputs(seed: int = 0) -> dict:
    key_of = jax.random.split(jax.random.key(seed), 7)
    tech = bell_draw(key_of[0], (SCENS, M, NX), (SCENS * M // 4) ** -0.5, 0.0234375, ((0, 32), (2, 4)))
    recourse = bell_draw(key_of[1], (SCENS, M, NY), M ** -0.5, 0.125, ((0, 32), (2, 4)))
    rhs = bell_draw(key_of[2], (BATCH, SCENS, M), 1.0, 6.0, ((1, 32),), jnp.float32)
    cost_first = bell_draw(key_of[3], (NX,), 1.0, 6.0, ((0, 4),), jnp.float32)
    cost_second = bell_draw(key_of[4], (SCENS, NY), 1.0, 6.0, ((0, 32), (1, 4)), jnp.float32)
    cone_id = jax.vmap(lambda own: jnp.searchsorted(jnp.cumsum(uneven_parts(own, NCONE, M, CONE_MOST, 2)), jnp.arange(M), side="right"))(jax.random.split(key_of[5], SCENS)).reshape((SCENS, M)).astype(jnp.int32)
    return dict(tech=tech, recourse=recourse, rhs=rhs, cost_first=cost_first, cost_second=cost_second, cone_id=cone_id)


HIGH = lax.Precision.HIGHEST

def cone_factors(lead, tail):
    norm_tail = jnp.sqrt(tail)
    inside = norm_tail <= lead
    polar = norm_tail <= -lead
    safe = jnp.where(norm_tail > 0.0, norm_tail, 1.0)
    middle = 0.5 * (lead + norm_tail)
    head = jnp.where(inside, lead, jnp.where(polar, 0.0, middle))
    scale = jnp.where(inside, 1.0, jnp.where(polar, 0.0, middle / safe))
    return (head, scale)

def reference(tech, recourse, rhs, cost_first, cost_second, cone_id):
    f32 = jnp.float32
    bf16 = jnp.bfloat16
    batch = rhs.shape[0]
    scen_count = tech.shape[0]
    rows = tech.shape[1]
    rhs_s = jnp.transpose(rhs, (1, 0, 2))
    starts = jnp.concatenate([jnp.ones((scen_count, 1), f32), (cone_id[:, 1:] != cone_id[:, :-1]).astype(f32)], axis=1)
    labels = lax.broadcasted_iota(jnp.int32, (1, 1, NCONE), 2)
    onehot = (cone_id[:, :, None] == labels).astype(f32)
    start_rows = starts[:, None, :]

    def project(values):
        lead = jnp.einsum('sbm,smc->sbc', values * start_rows, onehot, precision=HIGH)
        tail = jnp.einsum('sbm,smc->sbc', values * values * (1.0 - start_rows), onehot, precision=HIGH)
        head, scale = cone_factors(lead, tail)
        head_rows = jnp.einsum('sbc,smc->sbm', head, onehot, precision=HIGH)
        scale_rows = jnp.einsum('sbc,smc->sbm', scale, onehot, precision=HIGH)
        return start_rows * head_rows + (1.0 - start_rows) * values * scale_rows

    def forward(dir_first_bf, dir_second_bf):

        def single(args):
            tech_s, rec_s, dir_s = args
            return jnp.dot(dir_first_bf, tech_s.T, preferred_element_type=f32) + jnp.dot(dir_s, rec_s.T, preferred_element_type=f32)
        return lax.map(single, (tech, recourse, dir_second_bf))

    def adjoint(rows_bf):

        def single(carry, args):
            tech_s, rec_s, rows_s = args
            return (carry + jnp.dot(rows_s, tech_s, preferred_element_type=f32), jnp.dot(rows_s, rec_s, preferred_element_type=f32))
        return lax.scan(single, jnp.zeros((batch, tech.shape[2]), f32), (tech, recourse, rows_bf))

    def squares(first_vec, second_vec):
        return lax.optimization_barrier(jnp.sum(first_vec * first_vec, axis=1)) + lax.optimization_barrier(jnp.sum(second_vec * second_vec, axis=(0, 2)))
    first_sol = jnp.zeros((batch, tech.shape[2]), f32)
    second_sol = jnp.zeros((scen_count, batch, recourse.shape[2]), f32)
    slack = jnp.zeros((scen_count, batch, rows), f32)
    dual = jnp.zeros((scen_count, batch, rows), f32)
    image = jnp.zeros((scen_count, batch, rows), f32)
    for outer in range(ITERS):
        resid_rows = (rhs_s - slack - dual - image).astype(bf16)
        back_first, back_second = adjoint(resid_rows)
        res_first = back_first - cost_first[None, :]
        res_second = back_second - cost_second[:, None, :]
        res_norm = squares(res_first, res_second)
        dir_first, dir_second = (res_first, res_second)
        for step in range(CG_STEPS):
            image_step = forward(dir_first.astype(bf16), dir_second.astype(bf16))
            curv = squares(dir_first, dir_second) + lax.optimization_barrier(jnp.sum(image_step * image_step, axis=(0, 2)))
            alpha = res_norm / curv
            first_sol = first_sol + alpha[:, None] * dir_first
            second_sol = second_sol + alpha[None, :, None] * dir_second
            image = image + alpha[None, :, None] * image_step
            if step + 1 < CG_STEPS:
                back_first, back_second = adjoint(image_step.astype(bf16))
                res_first = res_first - alpha[:, None] * (dir_first + back_first)
                res_second = res_second - alpha[None, :, None] * (dir_second + back_second)
                new_norm = squares(res_first, res_second)
                ratio = new_norm / res_norm
                dir_first = res_first + ratio[:, None] * dir_first
                dir_second = res_second + ratio[None, :, None] * dir_second
                res_norm = new_norm
        slack = project(rhs_s - image - dual)
        dual = dual + image + slack - rhs_s
    return (first_sol, jnp.transpose(second_sol, (1, 0, 2)), jnp.transpose(slack, (1, 0, 2)), jnp.transpose(dual, (1, 0, 2)))
```

```python
import functools

import jax
import jax.numpy as jnp
from jax import lax
from jax.experimental import pallas as pl
from jax.experimental.pallas import tpu as pltpu
from jax.sharding import PartitionSpec as P

F32 = jnp.float32
BF16 = jnp.bfloat16
MESH = pl.DeviceIdType.MESH
NS = 32
NC = 4
BATCH = 32
ITERS = 3
CG_STEPS = 3
NCONE = 128
R = 1024
CH = 4


def dot(a, b):
    return jnp.dot(a, b, preferred_element_type=F32)


def dot_nt(a, b):
    return lax.dot_general(a, b, (((1,), (1,)), ((), ())), preferred_element_type=F32)


def two_parts(v):
    high = v.astype(BF16)
    return high, (v - high.astype(F32)).astype(BF16)


def fold(v):
    total = v[:, 0:128]
    for c in range(128, v.shape[1], 128):
        total = total + v[:, c : c + 128]
    return total


def kernel(
    tech, recourse, rhs, cost_first, cost_second, cone,
    first_out, second_out, slack_out, dual_out,
    T, W, rhs_v, image, dual, slack, q, own, pps, ppr, zs, zr, vown, vpart, bx, lx,
    onehot, starts, rx, dx, x, ry, dy, y, by, ly, rs_send, rs_recv, ag, xg, curv_all, norm_all,
    curv_col, norm_col, nres, alpha, beta, sq, sq_dir, fin,
    load_t, load_w, load_r, d2d_v, d2d_p, zsem, scen_sem, col_sem, fin_sem,
):
    me = lax.axis_index("scen")
    col = lax.axis_index("col")
    core = lax.rem(col, 2)
    partner = col + 1 - 2 * core
    across = lax.rem(col + 2, NC)
    bg = me // 8
    cg = lax.rem(me, 8)
    rows8 = pl.ds(pl.multiple_of(bg * 8, 8), 8)

    for i in range(CH):
        for half in range(2):
            scen = (core if half == 0 else 1 - core) * 2 + i // 2
            part = pl.ds((i % 2) * R, R)
            pltpu.make_async_copy(
                tech.at[scen, part], T.at[half * CH + i], load_t.at[half * CH + i]
            ).start()
        pltpu.make_async_copy(
            rhs.at[core * 2 + i // 2, :, pl.ds((i % 2) * R, R)], rhs_v.at[i], load_r.at[i]
        ).start()
    for i in range(CH):
        for half in range(2):
            scen = (core if half == 0 else 1 - core) * 2 + i // 2
            part = pl.ds((i % 2) * R, R)
            pltpu.make_async_copy(
                recourse.at[scen, part], W.at[half * CH + i], load_w.at[half * CH + i]
            ).start()

    barrier = pltpu.get_barrier_semaphore()
    for d in range(1, NS):
        pl.semaphore_signal(
            barrier, inc=1, device_id={"scen": lax.rem(me + d, NS)}, device_id_type=MESH
        )
    for d in range(1, NC):
        pl.semaphore_signal(
            barrier, inc=1, device_id={"col": lax.rem(col + d, NC)}, device_id_type=MESH
        )

    sub = lax.broadcasted_iota(jnp.int32, (BATCH, 128), 0)
    lane = lax.broadcasted_iota(jnp.int32, (BATCH, 128), 1)
    diag = sub == lane

    def to_row(v):
        column = jnp.sum(v, axis=1, keepdims=True)
        return jnp.sum(jnp.where(diag, column, 0.0), axis=0, keepdims=True)

    def to_columns(row):
        picked = jnp.where(diag, jnp.broadcast_to(row, (BATCH, 128)), 0.0)
        return jnp.broadcast_to(jnp.sum(picked, axis=1, keepdims=True), (BATCH, 128))

    def wide(v, n):
        return jnp.concatenate([v] * n, axis=1)

    def set_costs():
        rx[...] = -jnp.broadcast_to(cost_first[cg], (8, 128))
        dx[...] = jnp.zeros((8, 128), F32)
        for j in range(4):
            scen = (core if j < 2 else 1 - core) * 2 + j % 2
            ry[j] = -jnp.broadcast_to(cost_second[scen], (BATCH, 256))
            dy[j] = jnp.zeros((BATCH, 256), F32)

    for i in range(CH):
        image[i] = jnp.zeros((BATCH, R), F32)
        dual[i] = jnp.zeros((BATCH, R), F32)
        slack[i] = jnp.zeros((BATCH, R), F32)
        q[i] = jnp.zeros((BATCH, R), F32)
    x[...] = jnp.zeros((8, 128), F32)
    for j in range(4):
        y[j] = jnp.zeros((BATCH, 256), F32)
    nres[...] = jnp.ones((1, 128), F32)
    beta[...] = jnp.zeros((BATCH, 128), F32)
    set_costs()
    labels = lax.broadcasted_iota(jnp.int32, (NCONE, R), 0)
    row_lane = lax.broadcasted_iota(jnp.int32, (1, 2 * R), 1)
    for j in range(2):
        ids = cone[core * 2 + j]
        before = pltpu.roll(ids, 1, 1)
        fresh = jnp.where((row_lane == 0) | (ids != before), 1.0, 0.0)
        for p in range(2):
            starts[2 * j + p] = fresh[:, p * R : (p + 1) * R]
            here = ids[:, p * R : (p + 1) * R]
            onehot[2 * j + p] = jnp.where(
                jnp.broadcast_to(here, (NCONE, R)) == labels, 1.0, 0.0
            ).astype(BF16)

    for i in range(CH):
        pltpu.make_async_copy(rhs_v.at[i], rhs_v.at[i], load_r.at[i]).wait()
    pl.semaphore_wait(barrier, NS - 1 + NC - 1)

    def to_scens(source, target, sems):
        for d in range(1, NS):
            p = lax.rem(me + d, NS)
            pltpu.make_async_remote_copy(
                source(p), target.at[me], scen_sem.at[sems], scen_sem.at[sems + 1],
                device_id={"scen": p}, device_id_type=MESH,
            ).start()

    def all_came(buffer, sem):
        others = buffer.at[pl.ds(0, buffer.shape[0] - 1)]
        pltpu.make_async_copy(others, others, sem).wait()

    def to_cols(buffer, sems):
        for d in range(1, NC):
            p = lax.rem(col + d, NC)
            pltpu.make_async_remote_copy(
                buffer.at[col], buffer.at[col], col_sem.at[sems], col_sem.at[sems + 1],
                device_id={"col": p}, device_id_type=MESH,
            ).start()

    def rows_copy(i):
        return pltpu.make_async_remote_copy(
            vown.at[i], vpart.at[i], d2d_v.at[0, i], d2d_v.at[1, i],
            device_id={"col": partner}, device_id_type=MESH,
        )

    def partial_copy(i):
        return pltpu.make_async_remote_copy(
            pps.at[i], ppr.at[i], d2d_p.at[0, i], d2d_p.at[1, i],
            device_id={"col": partner}, device_id_type=MESH,
        )

    def across_copy(i):
        return pltpu.make_async_remote_copy(
            zs.at[i], zr.at[i], zsem.at[0, i], zsem.at[1, i],
            device_id={"col": across}, device_id_type=MESH,
        )

    def next_image_step(i):
        across_copy(i).wait()
        step = own[i] + zr[i].astype(F32) + wide(beta[...], R // 128) * q[i]
        q[i] = step
        sq[...] += fold(step * step)
        return step

    def curv_to_cols():
        curv_col[col] = to_row(0.5 * sq[...] + sq_dir[...])
        to_cols(curv_col, 0)

    def curv_to_scens():
        all_came(curv_col, col_sem.at[1])
        all_came(curv_col, col_sem.at[0])
        curv_all[me] = jnp.sum(curv_col[...], axis=0)
        to_scens(lambda p: curv_all.at[me], curv_all, 2)

    def set_alpha():
        all_came(curv_all, scen_sem.at[3])
        all_came(curv_all, scen_sem.at[2])
        alpha[...] = to_columns(nres[...] / jnp.sum(curv_all[...], axis=0))

    def add_steps():
        a = alpha[...]
        x[...] += alpha[rows8, :] * dx[...]
        for j in range(4):
            y[j] += wide(a, 2) * dy[j]
        for i in range(CH):
            image[i] += wide(a, R // 128) * q[i]

    def project():
        for j in range(2):
            sums = jnp.zeros((4 * BATCH, NCONE), F32)
            for i in (2 * j, 2 * j + 1):
                values = rhs_v[i] - image[i] - dual[i]
                start = jnp.broadcast_to(starts[i], (BATCH, R))
                lead_high, lead_low = two_parts(values * start)
                tail_high, tail_low = two_parts(values * values * (1.0 - start))
                stacked = jnp.concatenate([lead_high, lead_low, tail_high, tail_low], axis=0)
                sums = sums + dot_nt(stacked, onehot[i])
            lead = sums[0:32] + sums[32:64]
            norm_tail = jnp.sqrt(jnp.maximum(sums[64:96] + sums[96:128], 0.0))
            inside = norm_tail <= lead
            polar = norm_tail <= -lead
            safe = jnp.where(norm_tail > 0.0, norm_tail, 1.0)
            middle = 0.5 * (lead + norm_tail)
            head = jnp.where(inside, lead, jnp.where(polar, 0.0, middle))
            scale = jnp.where(inside, 1.0, jnp.where(polar, 0.0, middle / safe))
            factors = jnp.concatenate([*two_parts(head), *two_parts(scale)], axis=0)
            for i in (2 * j, 2 * j + 1):
                values = rhs_v[i] - image[i] - dual[i]
                start = jnp.broadcast_to(starts[i], (BATCH, R))
                spread = dot(factors, onehot[i])
                kept = values * (spread[64:96] + spread[96:128])
                new = jnp.where(start > 0.5, spread[0:32] + spread[32:64], kept)
                slack[i] = new
                dual[i] = dual[i] + image[i] + new - rhs_v[i]

    def iteration(t, carry):
        k = lax.rem(t, CG_STEPS)
        first = k == 0
        sq[...] = jnp.zeros((BATCH, 128), F32)

        def theirs(i):
            rows_copy(i).wait_recv()

            @pl.when(t == 0)
            def _():
                pltpu.make_async_copy(T.at[CH + i], T.at[CH + i], load_t.at[CH + i]).wait()

            return dot(vpart[i], T[CH + i])

        for i in range(CH):

            @pl.when(first)
            def _(i=i):
                vown[i] = (rhs_v[i] - slack[i] - dual[i] - image[i]).astype(BF16)

            @pl.when(jnp.logical_not(first))
            def _(i=i):
                vown[i] = next_image_step(i).astype(BF16)

            rows_copy(i).start()

            @pl.when(t == 0)
            def _(i=i):
                pltpu.make_async_copy(T.at[i], T.at[i], load_t.at[i]).wait()

            if i == 0:
                bx[...] = dot(vown[i], T[i])
            else:
                bx[...] += dot(vown[i], T[i])
                bx[...] += theirs(i - 1)

        @pl.when(jnp.logical_not(first))
        def _():
            curv_to_cols()

        total = bx[...] + theirs(CH - 1)
        for b in range(4):
            for c in range(8):
                rs_send[b * 8 + c] = total[b * 8 : b * 8 + 8, c * 128 : c * 128 + 128]
        to_scens(lambda p: rs_send.at[p], rs_recv, 0)
        rs_recv[me] = rs_send[me]

        @pl.when(jnp.logical_not(first))
        def _():
            curv_to_scens()

        @pl.when(t == 0)
        def _():
            for i in range(2 * CH):
                pltpu.make_async_copy(W.at[i], W.at[i], load_w.at[i]).wait()

        for j in range(4):
            rows = vown if j < 2 else vpart
            a = 2 * (j % 2)
            by[j] = dot(rows[a], W[2 * j]) + dot(rows[a + 1], W[2 * j + 1])

        @pl.when(first)
        def _():
            alpha[...] = jnp.full((BATCH, 128), -1.0, F32)

        @pl.when(jnp.logical_not(first))
        def _():
            set_alpha()

        all_came(rs_recv, scen_sem.at[1])
        back = jnp.sum(rs_recv[...], axis=0)
        res = rx[...] - alpha[rows8, :] * (dx[...] + back)
        rx[...] = res
        ag[me] = res.astype(BF16)
        to_scens(lambda p: ag.at[me], ag, 4)
        all_came(rs_send, scen_sem.at[0])

        norm = jnp.zeros((BATCH, 128), F32)
        for j in range(4):
            r = ry[j] - wide(alpha[...], 2) * (dy[j] + by[j])
            ry[j] = r
            ly[j] = r.astype(BF16)
            norm = norm + fold(r * r)
        sq_dir[...] = norm
        sq_dir[rows8, :] += res * res
        norm_all[me] = to_row(sq_dir[...])
        to_scens(lambda p: norm_all.at[me], norm_all, 6)
        add_steps()
        for i in range(CH):
            rows_copy(i).wait_send()
        all_came(norm_all, scen_sem.at[7])
        all_came(norm_all, scen_sem.at[6])
        norm_col[col] = jnp.sum(norm_all[...], axis=0)
        to_cols(norm_col, 2)
        all_came(ag, scen_sem.at[5])
        all_came(ag, scen_sem.at[4])
        for b in range(4):
            for c in range(8):
                xg[b * 8 : b * 8 + 8, c * 128 : c * 128 + 128] = ag[b * 8 + c].astype(F32)
        lx[...] = xg[...].astype(BF16)

        def exchange(i):
            partial_copy(i).wait_recv()
            here = own[i] + ppr[i]
            own[i] = here
            zs[i] = here.astype(BF16)
            across_copy(i).start()

        for i in range(CH):
            pps[i] = dot_nt(lx[...], T[CH + i]) + dot_nt(ly[2 + i // 2], W[CH + i])
            partial_copy(i).start()
            own[i] = dot_nt(lx[...], T[i]) + dot_nt(ly[i // 2], W[i])
            if i:
                exchange(i - 1)
        exchange(CH - 1)

        all_came(norm_col, col_sem.at[3])
        all_came(norm_col, col_sem.at[2])
        new_norm = jnp.sum(norm_col[...], axis=0)

        @pl.when(first)
        def _():
            beta[...] = jnp.zeros((BATCH, 128), F32)
            for i in range(CH):
                q[i] = jnp.zeros((BATCH, R), F32)

        @pl.when(jnp.logical_not(first))
        def _():
            beta[...] = to_columns(new_norm / nres[...])

        nres[...] = new_norm
        norm = jnp.zeros((BATCH, 128), F32)
        for j in range(4):
            d = ry[j] + wide(beta[...], 2) * dy[j]
            dy[j] = d
            norm = norm + fold(d * d)
        sq_dir[...] = norm
        d = rx[...] + beta[rows8, :] * dx[...]
        dx[...] = d
        sq_dir[rows8, :] += d * d
        for i in range(CH):
            partial_copy(i).wait_send()

        @pl.when(k == CG_STEPS - 1)
        def _():
            sq[...] = jnp.zeros((BATCH, 128), F32)
            for i in range(CH):
                next_image_step(i)
            curv_to_cols()
            curv_to_scens()
            set_alpha()
            add_steps()

            @pl.when(t == ITERS * CG_STEPS - 1)
            def _():
                rs_recv[me] = x[...]
                to_scens(lambda p: rs_recv.at[me], rs_recv, 0)

            set_costs()
            for i in range(CH):
                q[i] = jnp.zeros((BATCH, R), F32)
            project()

        return carry

    lax.fori_loop(0, ITERS * CG_STEPS, iteration, 0)

    quarter = col // 2
    lanes_here = pl.ds(pl.multiple_of(core * 512, 128), 512)
    lanes_there = pl.ds(pl.multiple_of((1 - core) * 512, 128), 512)

    def last_copy(a, j):
        return pltpu.make_async_remote_copy(
            (slack, dual)[a].at[2 * j + quarter, :, lanes_there], fin.at[a, j],
            fin_sem.at[0, a, j], fin_sem.at[1, a, j],
            device_id={"col": partner}, device_id_type=MESH,
        )

    for a in range(2):
        for j in range(2):
            last_copy(a, j).start()
    for j in range(2):
        slack_out[core * 2 + j] = slack[2 * j + quarter, :, lanes_here]
        dual_out[core * 2 + j] = dual[2 * j + quarter, :, lanes_here]
        second_out[core * 2 + j] = y[j]
        second_out[(1 - core) * 2 + j] = y[2 + j]
    for a in range(2):
        for j in range(2):
            last_copy(a, j).wait()
            (slack_out, dual_out)[a][(1 - core) * 2 + j] = fin[a, j]
    all_came(rs_recv, scen_sem.at[1])
    all_came(rs_recv, scen_sem.at[0])
    for b in range(4):
        for c in range(8):
            first_out[b * 8 : b * 8 + 8, c * 128 : c * 128 + 128] = rs_recv[b * 8 + c]


def body(tech, recourse, rhs, cost_first, cost_second, cone_id):
    any_space = pl.BlockSpec(memory_space=pl.ANY)
    vmem = pl.BlockSpec(memory_space=pltpu.VMEM)
    rows_f32 = pltpu.VMEM((CH, BATCH, R), F32)
    rows_bf16 = pltpu.VMEM((CH, BATCH, R), BF16)
    block = pltpu.VMEM((8, 128), F32)
    ys = pltpu.VMEM((4, BATCH, 256), F32)
    dma = pltpu.SemaphoreType.DMA
    first, second, slack, dual = pl.pallas_call(
        kernel,
        out_shape=(
            jax.ShapeDtypeStruct((BATCH, 1024), F32),
            jax.ShapeDtypeStruct((4, BATCH, 256), F32),
            jax.ShapeDtypeStruct((4, BATCH, 512), F32),
            jax.ShapeDtypeStruct((4, BATCH, 512), F32),
        ),
        in_specs=[any_space, any_space, any_space, vmem, vmem, vmem],
        out_specs=(vmem, vmem, vmem, vmem),
        scratch_shapes=[
            pltpu.VMEM((2 * CH, R, 1024), BF16),
            pltpu.VMEM((2 * CH, R, 256), BF16),
            rows_f32, rows_f32, rows_f32, rows_f32, rows_f32,
            rows_f32, rows_f32, rows_f32,
            rows_bf16, rows_bf16, rows_bf16, rows_bf16,
            pltpu.VMEM((BATCH, 1024), F32),
            pltpu.VMEM((BATCH, 1024), BF16),
            pltpu.VMEM((CH, NCONE, R), BF16),
            pltpu.VMEM((CH, 1, R), F32),
            block, block, block,
            ys, ys, ys, ys,
            pltpu.VMEM((4, BATCH, 256), BF16),
            pltpu.VMEM((NS, 8, 128), F32),
            pltpu.VMEM((NS, 8, 128), F32),
            pltpu.VMEM((NS, 8, 128), BF16),
            pltpu.VMEM((BATCH, 1024), F32),
            pltpu.VMEM((NS, 1, 128), F32),
            pltpu.VMEM((NS, 1, 128), F32),
            pltpu.VMEM((NC, 1, 128), F32),
            pltpu.VMEM((NC, 1, 128), F32),
            pltpu.VMEM((1, 128), F32),
            pltpu.VMEM((BATCH, 128), F32),
            pltpu.VMEM((BATCH, 128), F32),
            pltpu.VMEM((BATCH, 128), F32),
            pltpu.VMEM((BATCH, 128), F32),
            pltpu.VMEM((2, 2, BATCH, 512), F32),
            dma((2 * CH,)), dma((2 * CH,)), dma((CH,)),
            dma((2, CH)), dma((2, CH)), dma((2, CH)),
            dma((8,)), dma((4,)), dma((2, 2, 2)),
        ],
        compiler_params=pltpu.CompilerParams(
            collective_id=0, has_side_effects=True, vmem_limit_bytes=60 * 2**20
        ),
    )(
        tech,
        recourse,
        jnp.transpose(rhs, (1, 0, 2)),
        cost_first.reshape(8, 1, 128),
        cost_second.reshape(4, 1, 256),
        cone_id.reshape(4, 1, 2048),
    )
    return (
        first,
        jnp.transpose(second, (1, 0, 2)),
        jnp.transpose(slack, (1, 0, 2)),
        jnp.transpose(dual, (1, 0, 2)),
    )


def solution(mesh):
    return jax.shard_map(
        body,
        mesh=mesh,
        in_specs=(
            P("scen", None, "col"),
            P("scen", None, "col"),
            P(None, "scen", None),
            P("col"),
            P("scen", "col"),
            P("scen", None),
        ),
        out_specs=(
            P(None, "col"),
            P(None, "scen", "col"),
            P(None, "scen", "col"),
            P(None, "scen", "col"),
        ),
        check_vma=False,
    )
```

```python
import functools

import jax
import jax.numpy as jnp
from jax import lax
from jax.experimental import pallas as pl
from jax.experimental.pallas import tpu as pltpu
from jax.sharding import PartitionSpec as P

F32 = jnp.float32
BF16 = jnp.bfloat16
MESH = pl.DeviceIdType.MESH
NS = 32
NP = 16
NC = 4
BATCH = 32
ITERS = 3
CG_STEPS = 3
NCONE = 128
R = 1024
CH = 4


def dot(a, b):
    return jnp.dot(a, b, preferred_element_type=F32)


def dot_nt(a, b):
    return lax.dot_general(a, b, (((1,), (1,)), ((), ())), preferred_element_type=F32)


def two_parts(v):
    high = v.astype(BF16)
    return high, (v - high.astype(F32)).astype(BF16)


def fold(v):
    total = v[:, 0:128]
    for c in range(128, v.shape[1], 128):
        total = total + v[:, c : c + 128]
    return total


def kernel(
    tech, recourse, rhs, cost_first, cost_second, cone,
    first_out, second_out, slack_out, dual_out,
    T, W, TT, WT, rhs_v, image, dual, slack, q, own, pps, ppr, zs, zr, vown, vpart, bx, lx,
    onehot, starts, rx, dx, x, ry, dy, y, by, ly, rs_send, rs_recv, ag, xg, curv_all, norm_all,
    q_row, dir_col, norm_col, nres, alpha, beta, sq, sq_dir, fin,
    load_t, load_w, load_r, d2d_v, d2d_p, zsem, scen_sem, col_sem, row_sem, fin_sem,
):
    me = lax.axis_index("scen")
    col = lax.axis_index("col")
    core = lax.rem(col, 2)
    partner = col + 1 - 2 * core
    across = lax.rem(col + 2, NC)
    plane = me // NP
    place = lax.rem(me, NP)
    cg = lax.rem(place, 8)
    rows16 = pl.ds(pl.multiple_of((place // 8) * 16, 16), 16)

    for i in range(CH):
        for half in range(2):
            scen = (core if half == 0 else 1 - core) * 2 + i // 2
            part = pl.ds((i % 2) * R, R)
            pltpu.make_async_copy(
                tech.at[scen, part], T.at[half * CH + i], load_t.at[half * CH + i]
            ).start()
        pltpu.make_async_copy(
            rhs.at[:, core * 2 + i // 2, pl.ds((i % 2) * R, R)], rhs_v.at[i], load_r.at[i]
        ).start()
    for i in range(CH):
        for half in range(2):
            scen = (core if half == 0 else 1 - core) * 2 + i // 2
            part = pl.ds((i % 2) * R, R)
            pltpu.make_async_copy(
                recourse.at[scen, part], W.at[half * CH + i], load_w.at[half * CH + i]
            ).start()

    barrier = pltpu.get_barrier_semaphore()
    for d in range(1, NS):
        pl.semaphore_signal(
            barrier, inc=1, device_id={"scen": lax.rem(me + d, NS)}, device_id_type=MESH
        )
    for d in range(1, NC):
        pl.semaphore_signal(
            barrier, inc=1, device_id={"col": lax.rem(col + d, NC)}, device_id_type=MESH
        )

    sub = lax.broadcasted_iota(jnp.int32, (BATCH, 128), 0)
    lane = lax.broadcasted_iota(jnp.int32, (BATCH, 128), 1)
    diag = sub == lane

    def to_row(v):
        column = jnp.sum(v, axis=1, keepdims=True)
        return jnp.sum(jnp.where(diag, column, 0.0), axis=0, keepdims=True)

    def to_columns(row):
        picked = jnp.where(diag, jnp.broadcast_to(row, (BATCH, 128)), 0.0)
        return jnp.broadcast_to(jnp.sum(picked, axis=1, keepdims=True), (BATCH, 128))

    def wide(v, n):
        return jnp.concatenate([v] * n, axis=1)

    def pick(ref, half, j):
        return jnp.where(half == 0, ref[j : j + 1, :], ref[2 + j : 3 + j, :])

    def set_costs():
        rx[...] = -jnp.broadcast_to(cost_first[cg], (16, 128))
        dx[...] = jnp.zeros((16, 128), F32)
        for j in range(4):
            cost = pick(cost_second, core if j < 2 else 1 - core, j % 2)
            ry[j] = -jnp.broadcast_to(cost, (BATCH, 256))
            dy[j] = jnp.zeros((BATCH, 256), F32)

    for i in range(CH):
        image[i] = jnp.zeros((BATCH, R), F32)
        dual[i] = jnp.zeros((BATCH, R), F32)
        slack[i] = jnp.zeros((BATCH, R), F32)
        q[i] = jnp.zeros((BATCH, R), F32)
    x[...] = jnp.zeros((16, 128), F32)
    for j in range(4):
        y[j] = jnp.zeros((BATCH, 256), F32)
    nres[...] = jnp.ones((1, 128), F32)
    beta[...] = jnp.zeros((BATCH, 128), F32)
    set_costs()
    labels = lax.broadcasted_iota(jnp.int32, (NCONE, R), 0)
    row_lane = lax.broadcasted_iota(jnp.int32, (1, 2 * R), 1)
    for j in range(2):
        ids = pick(cone, core, j)
        before = pltpu.roll(ids, 1, 1)
        fresh = jnp.where((row_lane == 0) | (ids != before), 1.0, 0.0)
        for p in range(2):
            starts[2 * j + p] = fresh[:, p * R : (p + 1) * R]
            here = ids[:, p * R : (p + 1) * R]
            onehot[2 * j + p] = jnp.where(
                jnp.broadcast_to(here, (NCONE, R)) == labels, 1.0, 0.0
            ).astype(BF16)

    for i in range(CH):
        pltpu.make_async_copy(rhs_v.at[i], rhs_v.at[i], load_r.at[i]).wait()
    pl.semaphore_wait(barrier, NS - 1 + NC - 1)

    def to_scens(source, target, sems):
        for d in range(1, NS):
            p = lax.rem(me + d, NS)
            pltpu.make_async_remote_copy(
                source(p), target.at[me], scen_sem.at[sems], scen_sem.at[sems + 1],
                device_id={"scen": p}, device_id_type=MESH,
            ).start()

    def to_plane(buffer, sems):
        for d in range(1, NP):
            p = plane * NP + lax.rem(place + d, NP)
            pltpu.make_async_remote_copy(
                buffer.at[place], buffer.at[place], scen_sem.at[sems], scen_sem.at[sems + 1],
                device_id={"scen": p}, device_id_type=MESH,
            ).start()

    def all_came(buffer, sem):
        others = buffer.at[pl.ds(0, buffer.shape[0] - 1)]
        pltpu.make_async_copy(others, others, sem).wait()

    def to_cols(buffer, sems):
        for d in range(1, NC):
            p = lax.rem(col + d, NC)
            pltpu.make_async_remote_copy(
                buffer.at[col], buffer.at[col], col_sem.at[sems], col_sem.at[sems + 1],
                device_id={"col": p}, device_id_type=MESH,
            ).start()

    def rows_copy(i):
        return pltpu.make_async_remote_copy(
            vown.at[i], vpart.at[i], d2d_v.at[0, i], d2d_v.at[1, i],
            device_id={"col": partner}, device_id_type=MESH,
        )

    def partial_copy(i):
        return pltpu.make_async_remote_copy(
            pps.at[i], ppr.at[i], d2d_p.at[0, i], d2d_p.at[1, i],
            device_id={"col": partner}, device_id_type=MESH,
        )

    def across_copy(i, turn):
        return pltpu.make_async_remote_copy(
            zs.at[i], zr.at[turn, i], zsem.at[0, i], zsem.at[1 + turn, i],
            device_id={"col": across}, device_id_type=MESH,
        )

    def next_image_step(i, turn):
        across_copy(i, turn).wait()
        step = own[i] + zr[turn, i].astype(F32) + wide(beta[...], R // 128) * q[i]
        q[i] = step
        sq[...] += fold(step * step)
        return step

    def row_copy():
        return pltpu.make_async_remote_copy(
            q_row.at[core], q_row.at[core], row_sem.at[0], row_sem.at[1],
            device_id={"col": partner}, device_id_type=MESH,
        )

    def curv_to_partner():
        q_row[core] = to_row(sq[...])
        row_copy().start()

    def curv_to_scens():
        all_came(dir_col, col_sem.at[1])
        all_came(dir_col, col_sem.at[0])
        row_copy().wait()
        curv_all[me] = jnp.sum(dir_col[...], axis=0) + jnp.sum(q_row[...], axis=0)
        to_scens(lambda p: curv_all.at[me], curv_all, 2)

    def set_alpha():
        all_came(curv_all, scen_sem.at[3])
        all_came(curv_all, scen_sem.at[2])
        alpha[...] = to_columns(nres[...] / jnp.sum(curv_all[...], axis=0))

    def add_steps():
        a = alpha[...]
        x[...] += alpha[rows16, :] * dx[...]
        for j in range(4):
            y[j] += wide(a, 2) * dy[j]
        for i in range(CH):
            image[i] += wide(a, R // 128) * q[i]

    def project():
        for j in range(2):
            sums = jnp.zeros((4 * BATCH, NCONE), F32)
            for i in (2 * j, 2 * j + 1):
                values = rhs_v[i] - image[i] - dual[i]
                start = jnp.broadcast_to(starts[i], (BATCH, R))
                lead_high, lead_low = two_parts(values * start)
                tail_high, tail_low = two_parts(values * values * (1.0 - start))
                stacked = jnp.concatenate([lead_high, lead_low, tail_high, tail_low], axis=0)
                sums = sums + dot_nt(stacked, onehot[i])
            lead = sums[0:32] + sums[32:64]
            norm_tail = jnp.sqrt(jnp.maximum(sums[64:96] + sums[96:128], 0.0))
            inside = norm_tail <= lead
            polar = norm_tail <= -lead
            safe = jnp.where(norm_tail > 0.0, norm_tail, 1.0)
            middle = 0.5 * (lead + norm_tail)
            head = jnp.where(inside, lead, jnp.where(polar, 0.0, middle))
            scale = jnp.where(inside, 1.0, jnp.where(polar, 0.0, middle / safe))
            factors = jnp.concatenate([*two_parts(head), *two_parts(scale)], axis=0)
            for i in (2 * j, 2 * j + 1):
                values = rhs_v[i] - image[i] - dual[i]
                start = jnp.broadcast_to(starts[i], (BATCH, R))
                spread = dot(factors, onehot[i])
                kept = values * (spread[64:96] + spread[96:128])
                new = jnp.where(start > 0.5, spread[0:32] + spread[32:64], kept)
                slack[i] = new
                dual[i] = dual[i] + image[i] + new - rhs_v[i]

    def iteration(t, carry):
        k = lax.rem(t, CG_STEPS)
        first = k == 0
        turn = lax.rem(t, 2)
        sq[...] = jnp.zeros((BATCH, 128), F32)

        def theirs(i):
            rows_copy(i).wait_recv()

            @pl.when(t == 0)
            def _():
                pltpu.make_async_copy(T.at[CH + i], T.at[CH + i], load_t.at[CH + i]).wait()

            return dot(vpart[i], T[CH + i])

        for i in range(CH):

            @pl.when(first)
            def _(i=i):
                vown[i] = (rhs_v[i] - slack[i] - dual[i] - image[i]).astype(BF16)

            @pl.when(jnp.logical_not(first))
            def _(i=i):
                vown[i] = next_image_step(i, 1 - turn).astype(BF16)

            rows_copy(i).start()

            @pl.when(t == 0)
            def _(i=i):
                pltpu.make_async_copy(T.at[i], T.at[i], load_t.at[i]).wait()

            if i == 0:
                bx[...] = dot(vown[i], T[i])
            else:
                bx[...] += dot(vown[i], T[i])
                bx[...] += theirs(i - 1)

        @pl.when(jnp.logical_not(first))
        def _():
            curv_to_partner()

        total = bx[...] + theirs(CH - 1)
        for b in range(2):
            for c in range(8):
                tile = total[b * 16 : b * 16 + 16, c * 128 : c * 128 + 128]
                rs_send[b * 8 + c] = tile.astype(BF16)
        to_scens(lambda p: rs_send.at[lax.rem(p, NP)], rs_recv, 0)
        rs_recv[me] = rs_send[place]

        @pl.when(jnp.logical_not(first))
        def _():
            curv_to_scens()

        @pl.when(t == 0)
        def _():
            for i in range(2 * CH):
                pltpu.make_async_copy(W.at[i], W.at[i], load_w.at[i]).wait()

            def turned(i, carry):
                for b in range(0, R, 256):
                    for c in range(0, 1024, 256):
                        TT[i, c : c + 256, b : b + 256] = T[i, b : b + 256, c : c + 256].T
                    WT[i, :, b : b + 256] = W[i, b : b + 256, :].T
                return carry

            lax.fori_loop(0, 2 * CH, turned, 0)

        for j in range(4):
            rows = vown if j < 2 else vpart
            a = 2 * (j % 2)
            by[j] = dot(rows[a], W[2 * j]) + dot(rows[a + 1], W[2 * j + 1])

        @pl.when(first)
        def _():
            alpha[...] = jnp.full((BATCH, 128), -1.0, F32)

        @pl.when(jnp.logical_not(first))
        def _():
            set_alpha()

        all_came(rs_recv, scen_sem.at[1])
        back = jnp.sum(rs_recv[...].astype(F32), axis=0)
        res = rx[...] - alpha[rows16, :] * (dx[...] + back)
        rx[...] = res
        ag[place] = res.astype(BF16)
        to_plane(ag, 4)
        all_came(rs_recv, scen_sem.at[0])

        norm = jnp.zeros((BATCH, 128), F32)
        for j in range(4):
            r = ry[j] - wide(alpha[...], 2) * (dy[j] + by[j])
            ry[j] = r
            ly[j] = r.astype(BF16)
            norm = norm + fold(r * r)
        sq_dir[...] = norm
        sq_dir[rows16, :] += 0.5 * (res * res)
        norm_all[me] = to_row(sq_dir[...])
        to_scens(lambda p: norm_all.at[me], norm_all, 6)
        add_steps()
        for i in range(CH):
            rows_copy(i).wait_send()
        for i in range(CH):
            pps[i] = dot(ly[2 + i // 2], WT[CH + i])
            own[i] = dot(ly[i // 2], WT[i])
        all_came(ag, scen_sem.at[5])
        all_came(ag, scen_sem.at[4])
        for b in range(2):
            for c in range(8):
                lx[b * 16 : b * 16 + 16, c * 128 : c * 128 + 128] = ag[b * 8 + c]

        def exchange(i):
            partial_copy(i).wait_recv()
            here = own[i] + ppr[i]
            own[i] = here
            zs[i] = here.astype(BF16)
            across_copy(i, turn).start()

        for i in range(CH):
            pps[i] += dot(lx[...], TT[CH + i])
            partial_copy(i).start()
            own[i] += dot(lx[...], TT[i])
            if i:
                exchange(i - 1)
            if i == 1:
                all_came(norm_all, scen_sem.at[7])
                all_came(norm_all, scen_sem.at[6])
                norm_col[col] = jnp.sum(norm_all[...], axis=0)
                to_cols(norm_col, 2)
        exchange(CH - 1)

        all_came(norm_col, col_sem.at[3])
        all_came(norm_col, col_sem.at[2])
        new_norm = jnp.sum(norm_col[...], axis=0)

        @pl.when(first)
        def _():
            beta[...] = jnp.zeros((BATCH, 128), F32)
            for i in range(CH):
                q[i] = jnp.zeros((BATCH, R), F32)

        @pl.when(jnp.logical_not(first))
        def _():
            beta[...] = to_columns(new_norm / nres[...])

        nres[...] = new_norm
        norm = jnp.zeros((BATCH, 128), F32)
        for j in range(4):
            d = ry[j] + wide(beta[...], 2) * dy[j]
            dy[j] = d
            norm = norm + fold(d * d)
        sq_dir[...] = norm
        d = rx[...] + beta[rows16, :] * dx[...]
        dx[...] = d
        sq_dir[rows16, :] += 0.5 * (d * d)
        dir_col[col] = to_row(sq_dir[...])
        to_cols(dir_col, 0)
        for i in range(CH):
            partial_copy(i).wait_send()

        @pl.when(k == CG_STEPS - 1)
        def _():
            sq[...] = jnp.zeros((BATCH, 128), F32)
            for i in range(CH):
                next_image_step(i, turn)
            curv_to_partner()
            curv_to_scens()
            set_alpha()
            add_steps()

            @pl.when(t == ITERS * CG_STEPS - 1)
            def _():
                xg[place] = x[...]
                to_plane(xg, 8)

            set_costs()
            for i in range(CH):
                q[i] = jnp.zeros((BATCH, R), F32)
            project()

        return carry

    lax.fori_loop(0, ITERS * CG_STEPS, iteration, 0)

    quarter = col // 2
    lanes_here = pl.ds(pl.multiple_of(core * 512, 128), 512)
    lanes_there = pl.ds(pl.multiple_of((1 - core) * 512, 128), 512)

    def last_copy(a, j):
        return pltpu.make_async_remote_copy(
            (slack, dual)[a].at[2 * j + quarter, :, lanes_there], fin.at[a, j],
            fin_sem.at[0, a, j], fin_sem.at[1, a, j],
            device_id={"col": partner}, device_id_type=MESH,
        )

    for a in range(2):
        for j in range(2):
            last_copy(a, j).start()
    for j in range(2):
        slack_out[core * 2 + j] = slack[2 * j + quarter, :, lanes_here]
        dual_out[core * 2 + j] = dual[2 * j + quarter, :, lanes_here]
        second_out[core * 2 + j] = y[j]
        second_out[(1 - core) * 2 + j] = y[2 + j]
    for a in range(2):
        for j in range(2):
            last_copy(a, j).wait()
            (slack_out, dual_out)[a][(1 - core) * 2 + j] = fin[a, j]
    all_came(xg, scen_sem.at[9])
    all_came(xg, scen_sem.at[8])
    for b in range(2):
        for c in range(8):
            first_out[b * 16 : b * 16 + 16, c * 128 : c * 128 + 128] = xg[b * 8 + c]


def finish(first, second, slack, dual, first_out, second_out, slack_out, dual_out):
    first_out[...] = first[...]
    for j in range(4):
        second_out[:, j, :] = second[j]
        slack_out[:, j, :] = slack[j]
        dual_out[:, j, :] = dual[j]


def body(tech, recourse, rhs, cost_first, cost_second, cone_id):
    any_space = pl.BlockSpec(memory_space=pl.ANY)
    vmem = pl.BlockSpec(memory_space=pltpu.VMEM)
    rows_f32 = pltpu.VMEM((CH, BATCH, R), F32)
    rows_bf16 = pltpu.VMEM((CH, BATCH, R), BF16)
    block = pltpu.VMEM((16, 128), F32)
    ys = pltpu.VMEM((4, BATCH, 256), F32)
    dma = pltpu.SemaphoreType.DMA
    first, second, slack, dual = pl.pallas_call(
        kernel,
        out_shape=(
            jax.ShapeDtypeStruct((BATCH, 1024), F32),
            jax.ShapeDtypeStruct((4, BATCH, 256), F32),
            jax.ShapeDtypeStruct((4, BATCH, 512), F32),
            jax.ShapeDtypeStruct((4, BATCH, 512), F32),
        ),
        in_specs=[any_space, any_space, any_space, vmem, vmem, vmem],
        out_specs=(vmem, vmem, vmem, vmem),
        scratch_shapes=[
            pltpu.VMEM((2 * CH, R, 1024), BF16),
            pltpu.VMEM((2 * CH, R, 256), BF16),
            pltpu.VMEM((2 * CH, 1024, R), BF16),
            pltpu.VMEM((2 * CH, 256, R), BF16),
            rows_f32, rows_f32, rows_f32, rows_f32, rows_f32,
            rows_f32, rows_f32, rows_f32,
            rows_bf16, pltpu.VMEM((2, CH, BATCH, R), BF16),
            rows_bf16, rows_bf16,
            pltpu.VMEM((BATCH, 1024), F32),
            pltpu.VMEM((BATCH, 1024), BF16),
            pltpu.VMEM((CH, NCONE, R), BF16),
            pltpu.VMEM((CH, 1, R), F32),
            block, block, block,
            ys, ys, ys, ys,
            pltpu.VMEM((4, BATCH, 256), BF16),
            pltpu.VMEM((NP, 16, 128), BF16),
            pltpu.VMEM((NS, 16, 128), BF16),
            pltpu.VMEM((NP, 16, 128), BF16),
            pltpu.VMEM((NP, 16, 128), F32),
            pltpu.VMEM((NS, 1, 128), F32),
            pltpu.VMEM((NS, 1, 128), F32),
            pltpu.VMEM((2, 1, 128), F32),
            pltpu.VMEM((NC, 1, 128), F32),
            pltpu.VMEM((NC, 1, 128), F32),
            pltpu.VMEM((1, 128), F32),
            pltpu.VMEM((BATCH, 128), F32),
            pltpu.VMEM((BATCH, 128), F32),
            pltpu.VMEM((BATCH, 128), F32),
            pltpu.VMEM((BATCH, 128), F32),
            pltpu.VMEM((2, 2, BATCH, 512), F32),
            dma((2 * CH,)), dma((2 * CH,)), dma((CH,)),
            dma((2, CH)), dma((2, CH)), dma((3, CH)),
            dma((10,)), dma((4,)), dma((2,)), dma((2, 2, 2)),
        ],
        compiler_params=pltpu.CompilerParams(
            collective_id=0, has_side_effects=True, vmem_limit_bytes=60 * 2**20
        ),
    )(
        tech,
        recourse,
        rhs,
        cost_first.reshape(8, 1, 128),
        cost_second,
        cone_id,
    )
    return pl.pallas_call(
        finish,
        out_shape=(
            jax.ShapeDtypeStruct((BATCH, 1024), F32),
            jax.ShapeDtypeStruct((BATCH, 4, 256), F32),
            jax.ShapeDtypeStruct((BATCH, 4, 512), F32),
            jax.ShapeDtypeStruct((BATCH, 4, 512), F32),
        ),
        in_specs=[vmem, vmem, vmem, vmem],
        out_specs=(vmem, vmem, vmem, vmem),
    )(first, second, slack, dual)


def solution(mesh):
    return jax.shard_map(
        body,
        mesh=mesh,
        in_specs=(
            P("scen", None, "col"),
            P("scen", None, "col"),
            P(None, "scen", None),
            P("col"),
            P("scen", "col"),
            P("scen", None),
        ),
        out_specs=(
            P(None, "col"),
            P(None, "scen", "col"),
            P(None, "scen", "col"),
            P(None, "scen", "col"),
        ),
        check_vma=False,
    )
```

```python
import functools

import jax
import jax.numpy as jnp
from jax import lax
from jax.experimental import pallas as pl
from jax.experimental.pallas import tpu as pltpu
from jax.sharding import PartitionSpec as P

F32 = jnp.float32
BF16 = jnp.bfloat16
MESH = pl.DeviceIdType.MESH
NS = 32
NP = 16
NC = 4
BATCH = 32
ITERS = 3
CG_STEPS = 3
NCONE = 128
R = 1024
PER = 2048 // R
CH = 2 * PER
STEPS = sorted(
    ((z, x, y) for z in range(2) for x in range(4) for y in range(4) if z + x + y),
    key=lambda s: -(2 * s[0] + min(s[1], 4 - s[1]) + min(s[2], 4 - s[2])),
)


def dot(a, b):
    return jnp.dot(a, b, preferred_element_type=F32)


def dot_nt(a, b):
    return lax.dot_general(a, b, (((1,), (1,)), ((), ())), preferred_element_type=F32)


def two_parts(v):
    high = v.astype(BF16)
    return high, (v - high.astype(F32)).astype(BF16)


def fold(v):
    total = v[:, 0:128]
    for c in range(128, v.shape[1], 128):
        total = total + v[:, c : c + 128]
    return total


def kernel(
    tech, recourse, rhs, cost_first, cost_second, cone,
    first_out, second_out, slack_out, dual_out,
    T, W, TT, WT, rhs_v, image, dual, slack, q, own, pps, ppr, zs, zr, vown, vpart, bx, lx,
    onehot, starts, rx, dx, x, ry, dy, y, by, ly, rs_send, rs_recv, ag, xg, curv_all, norm_all,
    q_row, dir_col, norm_col, nres, alpha, beta, sq, sq_dir, fin,
    load_t, load_w, load_r, d2d_v, d2d_p, zsem, scen_sem, col_sem, row_sem, fin_sem,
):
    me = lax.axis_index("scen")
    col = lax.axis_index("col")
    core = lax.rem(col, 2)
    partner = col + 1 - 2 * core
    across = lax.rem(col + 2, NC)
    plane = me // NP
    place = lax.rem(me, NP)
    cg = lax.rem(place, 8)
    rows16 = pl.ds(pl.multiple_of((place // 8) * 16, 16), 16)

    for i in range(CH):
        for half in range(2):
            scen = (core if half == 0 else 1 - core) * 2 + i // PER
            part = pl.ds((i % PER) * R, R)
            pltpu.make_async_copy(
                tech.at[scen, part], T.at[half * CH + i], load_t.at[half * CH + i]
            ).start()
        pltpu.make_async_copy(
            rhs.at[:, core * 2 + i // PER, pl.ds((i % PER) * R, R)], rhs_v.at[i], load_r.at[i]
        ).start()
    for i in range(CH):
        for half in range(2):
            scen = (core if half == 0 else 1 - core) * 2 + i // PER
            part = pl.ds((i % PER) * R, R)
            pltpu.make_async_copy(
                recourse.at[scen, part], W.at[half * CH + i], load_w.at[half * CH + i]
            ).start()

    barrier = pltpu.get_barrier_semaphore()
    for d in range(1, NS):
        pl.semaphore_signal(
            barrier, inc=1, device_id={"scen": lax.rem(me + d, NS)}, device_id_type=MESH
        )
    for d in range(1, NC):
        pl.semaphore_signal(
            barrier, inc=1, device_id={"col": lax.rem(col + d, NC)}, device_id_type=MESH
        )

    sub = lax.broadcasted_iota(jnp.int32, (BATCH, 128), 0)
    lane = lax.broadcasted_iota(jnp.int32, (BATCH, 128), 1)
    diag = sub == lane

    def to_row(v):
        column = jnp.sum(v, axis=1, keepdims=True)
        return jnp.sum(jnp.where(diag, column, 0.0), axis=0, keepdims=True)

    def to_columns(row):
        picked = jnp.where(diag, jnp.broadcast_to(row, (BATCH, 128)), 0.0)
        return jnp.broadcast_to(jnp.sum(picked, axis=1, keepdims=True), (BATCH, 128))

    def wide(v, n):
        return jnp.concatenate([v] * n, axis=1)

    def pick(ref, half, j):
        return jnp.where(half == 0, ref[j : j + 1, :], ref[2 + j : 3 + j, :])

    def set_costs():
        rx[...] = -jnp.broadcast_to(cost_first[cg], (16, 128))
        dx[...] = jnp.zeros((16, 128), F32)
        for j in range(4):
            cost = pick(cost_second, core if j < 2 else 1 - core, j % 2)
            ry[j] = -jnp.broadcast_to(cost, (BATCH, 256))
            dy[j] = jnp.zeros((BATCH, 256), F32)

    for i in range(CH):
        image[i] = jnp.zeros((BATCH, R), F32)
        dual[i] = jnp.zeros((BATCH, R), F32)
        slack[i] = jnp.zeros((BATCH, R), F32)
        q[i] = jnp.zeros((BATCH, R), F32)
    x[...] = jnp.zeros((16, 128), F32)
    for j in range(4):
        y[j] = jnp.zeros((BATCH, 256), F32)
    nres[...] = jnp.ones((1, 128), F32)
    beta[...] = jnp.zeros((BATCH, 128), F32)
    set_costs()
    labels = lax.broadcasted_iota(jnp.int32, (NCONE, R), 0)
    row_lane = lax.broadcasted_iota(jnp.int32, (1, PER * R), 1)
    for j in range(2):
        ids = pick(cone, core, j)
        before = pltpu.roll(ids, 1, 1)
        fresh = jnp.where((row_lane == 0) | (ids != before), 1.0, 0.0)
        for p in range(PER):
            starts[PER * j + p] = fresh[:, p * R : (p + 1) * R]
            here = ids[:, p * R : (p + 1) * R]
            onehot[PER * j + p] = jnp.where(
                jnp.broadcast_to(here, (NCONE, R)) == labels, 1.0, 0.0
            ).astype(BF16)

    for i in range(CH):
        pltpu.make_async_copy(rhs_v.at[i], rhs_v.at[i], load_r.at[i]).wait()
    pl.semaphore_wait(barrier, NS - 1 + NC - 1)

    def other(step):
        z, x, y = step
        across_x = lax.rem(place // 4 + x, 4)
        across_y = lax.rem(lax.rem(place, 4) + y, 4)
        return lax.rem(plane + z, 2) * NP + across_x * 4 + across_y

    def to_scens(source, target, sems):
        for step in STEPS:
            p = other(step)
            pltpu.make_async_remote_copy(
                source(p), target.at[me], scen_sem.at[sems], scen_sem.at[sems + 1],
                device_id={"scen": p}, device_id_type=MESH,
            ).start()

    def to_plane(buffer, sems):
        for step in STEPS:
            if step[0]:
                continue
            p = other(step)
            pltpu.make_async_remote_copy(
                buffer.at[place], buffer.at[place], scen_sem.at[sems], scen_sem.at[sems + 1],
                device_id={"scen": p}, device_id_type=MESH,
            ).start()

    def all_came(buffer, sem):
        others = buffer.at[pl.ds(0, buffer.shape[0] - 1)]
        pltpu.make_async_copy(others, others, sem).wait()

    def to_cols(buffer, sems):
        for d in range(1, NC):
            p = lax.rem(col + d, NC)
            pltpu.make_async_remote_copy(
                buffer.at[col], buffer.at[col], col_sem.at[sems], col_sem.at[sems + 1],
                device_id={"col": p}, device_id_type=MESH,
            ).start()

    def rows_copy(i):
        return pltpu.make_async_remote_copy(
            vown.at[i], vpart.at[i], d2d_v.at[0, i], d2d_v.at[1, i],
            device_id={"col": partner}, device_id_type=MESH,
        )

    def partial_copy(i):
        return pltpu.make_async_remote_copy(
            pps.at[i], ppr.at[i], d2d_p.at[0, i], d2d_p.at[1, i],
            device_id={"col": partner}, device_id_type=MESH,
        )

    def across_copy(i, turn):
        return pltpu.make_async_remote_copy(
            zs.at[i], zr.at[turn, i], zsem.at[0, i], zsem.at[1 + turn, i],
            device_id={"col": across}, device_id_type=MESH,
        )

    def next_image_step(i, turn):
        across_copy(i, turn).wait()
        step = own[i] + zr[turn, i].astype(F32) + wide(beta[...], R // 128) * q[i]
        q[i] = step
        sq[...] += fold(step * step)
        return step

    def row_copy():
        return pltpu.make_async_remote_copy(
            q_row.at[core], q_row.at[core], row_sem.at[0], row_sem.at[1],
            device_id={"col": partner}, device_id_type=MESH,
        )

    def curv_to_partner():
        q_row[core] = to_row(sq[...])
        row_copy().start()

    def curv_to_scens():
        all_came(dir_col, col_sem.at[1])
        all_came(dir_col, col_sem.at[0])
        row_copy().wait()
        curv_all[me] = jnp.sum(dir_col[...], axis=0) + jnp.sum(q_row[...], axis=0)
        to_scens(lambda p: curv_all.at[me], curv_all, 2)

    def set_alpha():
        all_came(curv_all, scen_sem.at[3])
        all_came(curv_all, scen_sem.at[2])
        alpha[...] = to_columns(nres[...] / jnp.sum(curv_all[...], axis=0))

    def add_steps():
        a = alpha[...]
        x[...] += alpha[rows16, :] * dx[...]
        for j in range(4):
            y[j] += wide(a, 2) * dy[j]
        for i in range(CH):
            image[i] += wide(a, R // 128) * q[i]

    def project():
        for j in range(2):
            sums = jnp.zeros((4 * BATCH, NCONE), F32)
            for i in range(PER * j, PER * j + PER):
                values = rhs_v[i] - image[i] - dual[i]
                start = jnp.broadcast_to(starts[i], (BATCH, R))
                lead_high, lead_low = two_parts(values * start)
                tail_high, tail_low = two_parts(values * values * (1.0 - start))
                stacked = jnp.concatenate([lead_high, lead_low, tail_high, tail_low], axis=0)
                sums = sums + dot_nt(stacked, onehot[i])
            lead = sums[0:32] + sums[32:64]
            norm_tail = jnp.sqrt(jnp.maximum(sums[64:96] + sums[96:128], 0.0))
            inside = norm_tail <= lead
            polar = norm_tail <= -lead
            safe = jnp.where(norm_tail > 0.0, norm_tail, 1.0)
            middle = 0.5 * (lead + norm_tail)
            head = jnp.where(inside, lead, jnp.where(polar, 0.0, middle))
            scale = jnp.where(inside, 1.0, jnp.where(polar, 0.0, middle / safe))
            factors = jnp.concatenate([*two_parts(head), *two_parts(scale)], axis=0)
            for i in range(PER * j, PER * j + PER):
                values = rhs_v[i] - image[i] - dual[i]
                start = jnp.broadcast_to(starts[i], (BATCH, R))
                spread = dot(factors, onehot[i])
                kept = values * (spread[64:96] + spread[96:128])
                new = jnp.where(start > 0.5, spread[0:32] + spread[32:64], kept)
                slack[i] = new
                dual[i] = dual[i] + image[i] + new - rhs_v[i]

    def iteration(t, carry):
        k = lax.rem(t, CG_STEPS)
        first = k == 0
        turn = lax.rem(t, 2)
        sq[...] = jnp.zeros((BATCH, 128), F32)

        def theirs(i):
            rows_copy(i).wait_recv()

            @pl.when(t == 0)
            def _():
                pltpu.make_async_copy(T.at[CH + i], T.at[CH + i], load_t.at[CH + i]).wait()

            return dot(vpart[i], T[CH + i])

        for i in range(CH):

            @pl.when(first)
            def _(i=i):
                vown[i] = (rhs_v[i] - slack[i] - dual[i] - image[i]).astype(BF16)

            @pl.when(jnp.logical_not(first))
            def _(i=i):
                vown[i] = next_image_step(i, 1 - turn).astype(BF16)

            rows_copy(i).start()

            if i == CH - 1:

                @pl.when(jnp.logical_not(first))
                def _():
                    curv_to_partner()

            @pl.when(t == 0)
            def _(i=i):
                pltpu.make_async_copy(T.at[i], T.at[i], load_t.at[i]).wait()

            if i == 0:
                bx[...] = dot(vown[i], T[i])
            else:
                bx[...] += dot(vown[i], T[i])
                bx[...] += theirs(i - 1)

        @pl.when(jnp.logical_not(first))
        def _():
            curv_to_scens()

        total = bx[...] + theirs(CH - 1)
        for b in range(2):
            for c in range(8):
                tile = total[b * 16 : b * 16 + 16, c * 128 : c * 128 + 128]
                rs_send[b * 8 + c] = tile.astype(BF16)
        to_scens(lambda p: rs_send.at[lax.rem(p, NP)], rs_recv, 0)
        rs_recv[me] = rs_send[place]

        @pl.when(t == 0)
        def _():
            for i in range(2 * CH):
                pltpu.make_async_copy(W.at[i], W.at[i], load_w.at[i]).wait()

            def turned(i, carry):
                for b in range(0, R, 256):
                    for c in range(0, 1024, 256):
                        TT[i, c : c + 256, b : b + 256] = T[i, b : b + 256, c : c + 256].T
                    WT[i, :, b : b + 256] = W[i, b : b + 256, :].T
                return carry

            lax.fori_loop(0, 2 * CH, turned, 0)

        for j in range(4):
            rows = vown if j < 2 else vpart
            a = PER * (j % 2)
            by[j] = sum(dot(rows[a + p], W[PER * j + p]) for p in range(PER))

        @pl.when(first)
        def _():
            alpha[...] = jnp.full((BATCH, 128), -1.0, F32)

        @pl.when(jnp.logical_not(first))
        def _():
            set_alpha()

        norm = jnp.zeros((BATCH, 128), F32)
        for j in range(4):
            r = ry[j] - wide(alpha[...], 2) * (dy[j] + by[j])
            ry[j] = r
            ly[j] = r.astype(BF16)
            norm = norm + fold(r * r)
        sq_dir[...] = norm

        all_came(rs_recv, scen_sem.at[1])
        back = jnp.sum(rs_recv[...].astype(F32), axis=0)
        res = rx[...] - alpha[rows16, :] * (dx[...] + back)
        rx[...] = res
        ag[place] = res.astype(BF16)
        to_plane(ag, 4)
        sq_dir[rows16, :] += 0.5 * (res * res)
        norm_all[me] = to_row(sq_dir[...])
        to_scens(lambda p: norm_all.at[me], norm_all, 6)
        add_steps()
        all_came(rs_recv, scen_sem.at[0])
        for i in range(CH):
            rows_copy(i).wait_send()
        for i in range(CH):
            pps[i] = dot(ly[2 + i // PER], WT[CH + i])
            own[i] = dot(ly[i // PER], WT[i])
        all_came(ag, scen_sem.at[5])
        for b in range(2):
            for c in range(8):
                lx[b * 16 : b * 16 + 16, c * 128 : c * 128 + 128] = ag[b * 8 + c]

        def exchange(i):
            partial_copy(i).wait_recv()
            here = own[i] + ppr[i]
            own[i] = here
            zs[i] = here.astype(BF16)
            across_copy(i, turn).start()

        for i in range(CH):
            pps[i] += dot(lx[...], TT[CH + i])
            partial_copy(i).start()
            own[i] += dot(lx[...], TT[i])
            if i:
                exchange(i - 1)
            if i == PER // 2:
                all_came(norm_all, scen_sem.at[7])
                all_came(norm_all, scen_sem.at[6])
                norm_col[col] = jnp.sum(norm_all[...], axis=0)
                to_cols(norm_col, 2)
        exchange(CH - 1)

        all_came(ag, scen_sem.at[4])
        all_came(norm_col, col_sem.at[3])
        all_came(norm_col, col_sem.at[2])
        new_norm = jnp.sum(norm_col[...], axis=0)

        @pl.when(first)
        def _():
            beta[...] = jnp.zeros((BATCH, 128), F32)
            for i in range(CH):
                q[i] = jnp.zeros((BATCH, R), F32)

        @pl.when(jnp.logical_not(first))
        def _():
            beta[...] = to_columns(new_norm / nres[...])

        nres[...] = new_norm
        norm = jnp.zeros((BATCH, 128), F32)
        for j in range(4):
            d = ry[j] + wide(beta[...], 2) * dy[j]
            dy[j] = d
            norm = norm + fold(d * d)
        sq_dir[...] = norm
        d = rx[...] + beta[rows16, :] * dx[...]
        dx[...] = d
        sq_dir[rows16, :] += 0.5 * (d * d)
        dir_col[col] = to_row(sq_dir[...])
        to_cols(dir_col, 0)
        for i in range(CH):
            partial_copy(i).wait_send()

        @pl.when(k == CG_STEPS - 1)
        def _():
            sq[...] = jnp.zeros((BATCH, 128), F32)
            for i in range(CH):
                next_image_step(i, turn)
            curv_to_partner()
            curv_to_scens()
            set_alpha()
            add_steps()

            @pl.when(t == ITERS * CG_STEPS - 1)
            def _():
                xg[place] = x[...]
                to_plane(xg, 8)

            set_costs()
            for i in range(CH):
                q[i] = jnp.zeros((BATCH, R), F32)
            project()

        return carry

    lax.fori_loop(0, ITERS * CG_STEPS, iteration, 0)

    if PER == 2:
        here = there = col // 2
        lanes_here = pl.ds(pl.multiple_of(core * 512, 128), 512)
        lanes_there = pl.ds(pl.multiple_of((1 - core) * 512, 128), 512)
    else:
        here, there = col, partner
        lanes_here = lanes_there = slice(None)

    def last_copy(a, j):
        return pltpu.make_async_remote_copy(
            (slack, dual)[a].at[PER * j + there, :, lanes_there], fin.at[a, j],
            fin_sem.at[0, a, j], fin_sem.at[1, a, j],
            device_id={"col": partner}, device_id_type=MESH,
        )

    for a in range(2):
        for j in range(2):
            last_copy(a, j).start()
    for j in range(2):
        slack_out[core * 2 + j] = slack[PER * j + here, :, lanes_here]
        dual_out[core * 2 + j] = dual[PER * j + here, :, lanes_here]
        second_out[core * 2 + j] = y[j]
        second_out[(1 - core) * 2 + j] = y[2 + j]
    for a in range(2):
        for j in range(2):
            last_copy(a, j).wait()
            (slack_out, dual_out)[a][(1 - core) * 2 + j] = fin[a, j]
    all_came(xg, scen_sem.at[9])
    all_came(xg, scen_sem.at[8])
    for b in range(2):
        for c in range(8):
            first_out[b * 16 : b * 16 + 16, c * 128 : c * 128 + 128] = xg[b * 8 + c]


def finish(first, second, slack, dual, first_out, second_out, slack_out, dual_out):
    first_out[...] = first[...]
    for j in range(4):
        second_out[:, j, :] = second[j]
        slack_out[:, j, :] = slack[j]
        dual_out[:, j, :] = dual[j]


def body(tech, recourse, rhs, cost_first, cost_second, cone_id):
    any_space = pl.BlockSpec(memory_space=pl.ANY)
    vmem = pl.BlockSpec(memory_space=pltpu.VMEM)
    rows_f32 = pltpu.VMEM((CH, BATCH, R), F32)
    rows_bf16 = pltpu.VMEM((CH, BATCH, R), BF16)
    block = pltpu.VMEM((16, 128), F32)
    ys = pltpu.VMEM((4, BATCH, 256), F32)
    dma = pltpu.SemaphoreType.DMA
    first, second, slack, dual = pl.pallas_call(
        kernel,
        out_shape=(
            jax.ShapeDtypeStruct((BATCH, 1024), F32),
            jax.ShapeDtypeStruct((4, BATCH, 256), F32),
            jax.ShapeDtypeStruct((4, BATCH, 512), F32),
            jax.ShapeDtypeStruct((4, BATCH, 512), F32),
        ),
        in_specs=[any_space, any_space, any_space, vmem, vmem, vmem],
        out_specs=(vmem, vmem, vmem, vmem),
        scratch_shapes=[
            pltpu.VMEM((2 * CH, R, 1024), BF16),
            pltpu.VMEM((2 * CH, R, 256), BF16),
            pltpu.VMEM((2 * CH, 1024, R), BF16),
            pltpu.VMEM((2 * CH, 256, R), BF16),
            rows_f32, rows_f32, rows_f32, rows_f32, rows_f32,
            rows_f32, rows_f32, rows_f32,
            rows_bf16, pltpu.VMEM((2, CH, BATCH, R), BF16),
            rows_bf16, rows_bf16,
            pltpu.VMEM((BATCH, 1024), F32),
            pltpu.VMEM((BATCH, 1024), BF16),
            pltpu.VMEM((CH, NCONE, R), BF16),
            pltpu.VMEM((CH, 1, R), F32),
            block, block, block,
            ys, ys, ys, ys,
            pltpu.VMEM((4, BATCH, 256), BF16),
            pltpu.VMEM((NP, 16, 128), BF16),
            pltpu.VMEM((NS, 16, 128), BF16),
            pltpu.VMEM((NP, 16, 128), BF16),
            pltpu.VMEM((NP, 16, 128), F32),
            pltpu.VMEM((NS, 1, 128), F32),
            pltpu.VMEM((NS, 1, 128), F32),
            pltpu.VMEM((2, 1, 128), F32),
            pltpu.VMEM((NC, 1, 128), F32),
            pltpu.VMEM((NC, 1, 128), F32),
            pltpu.VMEM((1, 128), F32),
            pltpu.VMEM((BATCH, 128), F32),
            pltpu.VMEM((BATCH, 128), F32),
            pltpu.VMEM((BATCH, 128), F32),
            pltpu.VMEM((BATCH, 128), F32),
            pltpu.VMEM((2, 2, BATCH, 512), F32),
            dma((2 * CH,)), dma((2 * CH,)), dma((CH,)),
            dma((2, CH)), dma((2, CH)), dma((3, CH)),
            dma((10,)), dma((4,)), dma((2,)), dma((2, 2, 2)),
        ],
        compiler_params=pltpu.CompilerParams(
            collective_id=0, has_side_effects=True, vmem_limit_bytes=60 * 2**20
        ),
    )(
        tech,
        recourse,
        rhs,
        cost_first.reshape(8, 1, 128),
        cost_second,
        cone_id,
    )
    return pl.pallas_call(
        finish,
        out_shape=(
            jax.ShapeDtypeStruct((BATCH, 1024), F32),
            jax.ShapeDtypeStruct((BATCH, 4, 256), F32),
            jax.ShapeDtypeStruct((BATCH, 4, 512), F32),
            jax.ShapeDtypeStruct((BATCH, 4, 512), F32),
        ),
        in_specs=[vmem, vmem, vmem, vmem],
        out_specs=(vmem, vmem, vmem, vmem),
    )(first, second, slack, dual)


def solution(mesh):
    return jax.shard_map(
        body,
        mesh=mesh,
        in_specs=(
            P("scen", None, "col"),
            P("scen", None, "col"),
            P(None, "scen", None),
            P("col"),
            P("scen", "col"),
            P("scen", None),
        ),
        out_specs=(
            P(None, "col"),
            P(None, "scen", "col"),
            P(None, "scen", "col"),
            P(None, "scen", "col"),
        ),
        check_vma=False,
    )
```

```python
import functools

import jax
import jax.numpy as jnp
from jax import lax
from jax.experimental import pallas as pl
from jax.experimental.pallas import tpu as pltpu
from jax.sharding import PartitionSpec as P

F32 = jnp.float32
BF16 = jnp.bfloat16
MESH = pl.DeviceIdType.MESH
NS = 32
NP = 16
NC = 4
BATCH = 32
ITERS = 3
CG_STEPS = 3
NCONE = 128
R = 1024
PER = 2048 // R
CH = 2 * PER
STEPS = sorted(
    ((z, x, y) for z in range(2) for x in range(4) for y in range(4) if z + x + y),
    key=lambda s: -(2 * s[0] + min(s[1], 4 - s[1]) + min(s[2], 4 - s[2])),
)


def dot(a, b):
    return jnp.dot(a, b, preferred_element_type=F32)


def dot_nt(a, b):
    return lax.dot_general(a, b, (((1,), (1,)), ((), ())), preferred_element_type=F32)


def two_parts(v):
    high = v.astype(BF16)
    return high, (v - high.astype(F32)).astype(BF16)


def fold(v):
    total = v[:, 0:128]
    for c in range(128, v.shape[1], 128):
        total = total + v[:, c : c + 128]
    return total


def kernel(
    tech, recourse, rhs, cost_first, cost_second, cone,
    first_out, second_out, slack_out, dual_out,
    T, W, TT, WT, rhs_v, image, dual, slack, q, own, pps, ppr, zs, zr, vown, vpart, bx, lx,
    onehot, starts, rx, dx, x, ry, dy, y, by, ly, rs_send, rs_recv, ag, xg, curv_all, norm_all,
    q_row, dir_col, norm_col, nres, alpha, beta, sq, sq_dir, fin,
    load_t, load_w, load_r, d2d_v, d2d_p, zsem, scen_sem, col_sem, row_sem, fin_sem,
):
    me = lax.axis_index("scen")
    col = lax.axis_index("col")
    core = lax.rem(col, 2)
    partner = col + 1 - 2 * core
    across = lax.rem(col + 2, NC)
    plane = me // NP
    place = lax.rem(me, NP)
    cg = lax.rem(place, 8)
    rows16 = pl.ds(pl.multiple_of((place // 8) * 16, 16), 16)

    def fetch(source, target, sem, i):
        scen = (core if i < CH else 1 - core) * 2 + i % CH // PER
        part = pl.ds((i % PER) * R, R)
        pltpu.make_async_copy(source.at[scen, part], target.at[i], sem.at[i]).start()

    for i in range(CH):
        pltpu.make_async_copy(
            rhs.at[:, core * 2 + i // PER, pl.ds((i % PER) * R, R)], rhs_v.at[i], load_r.at[i]
        ).start()
    for i in (0, 1, 2, 4, 5, 3, 6, 7):
        fetch(tech, T, load_t, i)
    for i in range(2 * CH):
        fetch(recourse, W, load_w, i)

    barrier = pltpu.get_barrier_semaphore()
    for d in range(1, NS):
        pl.semaphore_signal(
            barrier, inc=1, device_id={"scen": lax.rem(me + d, NS)}, device_id_type=MESH
        )
    for d in range(1, NC):
        pl.semaphore_signal(
            barrier, inc=1, device_id={"col": lax.rem(col + d, NC)}, device_id_type=MESH
        )

    sub = lax.broadcasted_iota(jnp.int32, (BATCH, 128), 0)
    lane = lax.broadcasted_iota(jnp.int32, (BATCH, 128), 1)
    diag = sub == lane

    def to_row(v):
        column = jnp.sum(v, axis=1, keepdims=True)
        return jnp.sum(jnp.where(diag, column, 0.0), axis=0, keepdims=True)

    def to_columns(row):
        picked = jnp.where(diag, jnp.broadcast_to(row, (BATCH, 128)), 0.0)
        return jnp.broadcast_to(jnp.sum(picked, axis=1, keepdims=True), (BATCH, 128))

    def wide(v, n):
        return jnp.concatenate([v] * n, axis=1)

    def pick(ref, half, j):
        return jnp.where(half == 0, ref[j : j + 1, :], ref[2 + j : 3 + j, :])

    def set_costs():
        rx[...] = -jnp.broadcast_to(cost_first[cg], (16, 128))
        dx[...] = jnp.zeros((16, 128), F32)
        for j in range(4):
            cost = pick(cost_second, core if j < 2 else 1 - core, j % 2)
            ry[j] = -jnp.broadcast_to(cost, (BATCH, 256))
            dy[j] = jnp.zeros((BATCH, 256), F32)

    for i in range(CH):
        image[i] = jnp.zeros((BATCH, R), F32)
        dual[i] = jnp.zeros((BATCH, R), F32)
        slack[i] = jnp.zeros((BATCH, R), F32)
        q[i] = jnp.zeros((BATCH, R), F32)
    x[...] = jnp.zeros((16, 128), F32)
    for j in range(4):
        y[j] = jnp.zeros((BATCH, 256), F32)
    nres[...] = jnp.ones((1, 128), F32)
    beta[...] = jnp.zeros((BATCH, 128), F32)
    set_costs()
    labels = lax.broadcasted_iota(jnp.int32, (NCONE, R), 0)
    row_lane = lax.broadcasted_iota(jnp.int32, (1, PER * R), 1)
    for j in range(2):
        ids = pick(cone, core, j)
        before = pltpu.roll(ids, 1, 1)
        fresh = jnp.where((row_lane == 0) | (ids != before), 1.0, 0.0)
        for p in range(PER):
            starts[PER * j + p] = fresh[:, p * R : (p + 1) * R]
            here = ids[:, p * R : (p + 1) * R]
            onehot[PER * j + p] = jnp.where(
                jnp.broadcast_to(here, (NCONE, R)) == labels, 1.0, 0.0
            ).astype(BF16)

    for i in range(CH):
        pltpu.make_async_copy(rhs_v.at[i], rhs_v.at[i], load_r.at[i]).wait()
    pl.semaphore_wait(barrier, NS - 1 + NC - 1)

    def other(step):
        z, x, y = step
        across_x = lax.rem(place // 4 + x, 4)
        across_y = lax.rem(lax.rem(place, 4) + y, 4)
        return lax.rem(plane + z, 2) * NP + across_x * 4 + across_y

    others = [other(step) for step in STEPS]

    def to_scens(source, target, sems):
        for p in others:
            pltpu.make_async_remote_copy(
                source(p), target.at[me], scen_sem.at[sems], scen_sem.at[sems + 1],
                device_id={"scen": p}, device_id_type=MESH,
            ).start()

    def to_plane(buffer, sems):
        for step, p in zip(STEPS, others):
            if step[0]:
                continue
            pltpu.make_async_remote_copy(
                buffer.at[place], buffer.at[place], scen_sem.at[sems], scen_sem.at[sems + 1],
                device_id={"scen": p}, device_id_type=MESH,
            ).start()

    def all_came(buffer, sem):
        others = buffer.at[pl.ds(0, buffer.shape[0] - 1)]
        pltpu.make_async_copy(others, others, sem).wait()

    def to_cols(buffer, sems):
        for d in range(1, NC):
            p = lax.rem(col + d, NC)
            pltpu.make_async_remote_copy(
                buffer.at[col], buffer.at[col], col_sem.at[sems], col_sem.at[sems + 1],
                device_id={"col": p}, device_id_type=MESH,
            ).start()

    def rows_copy(i):
        return pltpu.make_async_remote_copy(
            vown.at[i], vpart.at[i], d2d_v.at[0, i], d2d_v.at[1, i],
            device_id={"col": partner}, device_id_type=MESH,
        )

    def partial_copy(i):
        return pltpu.make_async_remote_copy(
            pps.at[i], ppr.at[i], d2d_p.at[0, i], d2d_p.at[1, i],
            device_id={"col": partner}, device_id_type=MESH,
        )

    def across_copy(i, turn):
        return pltpu.make_async_remote_copy(
            zs.at[i], zr.at[turn, i], zsem.at[0, i], zsem.at[1 + turn, i],
            device_id={"col": across}, device_id_type=MESH,
        )

    def next_image_step(i, turn):
        across_copy(i, turn).wait()
        step = own[i] + zr[turn, i].astype(F32) + wide(beta[...], R // 128) * q[i]
        q[i] = step
        sq[...] += fold(step * step)
        return step

    def row_copy():
        return pltpu.make_async_remote_copy(
            q_row.at[core], q_row.at[core], row_sem.at[0], row_sem.at[1],
            device_id={"col": partner}, device_id_type=MESH,
        )

    def curv_to_partner():
        q_row[core] = to_row(sq[...])
        row_copy().start()

    def curv_to_scens():
        all_came(dir_col, col_sem.at[1])
        all_came(dir_col, col_sem.at[0])
        row_copy().wait()
        curv_all[me] = jnp.sum(dir_col[...], axis=0) + jnp.sum(q_row[...], axis=0)
        to_scens(lambda p: curv_all.at[me], curv_all, 2)

    def set_alpha():
        all_came(curv_all, scen_sem.at[3])
        all_came(curv_all, scen_sem.at[2])
        alpha[...] = to_columns(nres[...] / jnp.sum(curv_all[...], axis=0))

    def add_steps():
        a = alpha[...]
        x[...] += alpha[rows16, :] * dx[...]
        for j in range(4):
            y[j] += wide(a, 2) * dy[j]
        for i in range(CH):
            image[i] += wide(a, R // 128) * q[i]

    def project():
        for j in range(2):
            sums = jnp.zeros((4 * BATCH, NCONE), F32)
            for i in range(PER * j, PER * j + PER):
                values = rhs_v[i] - image[i] - dual[i]
                start = jnp.broadcast_to(starts[i], (BATCH, R))
                lead_high, lead_low = two_parts(values * start)
                tail_high, tail_low = two_parts(values * values * (1.0 - start))
                stacked = jnp.concatenate([lead_high, lead_low, tail_high, tail_low], axis=0)
                sums = sums + dot_nt(stacked, onehot[i])
            lead = sums[0:32] + sums[32:64]
            norm_tail = jnp.sqrt(jnp.maximum(sums[64:96] + sums[96:128], 0.0))
            inside = norm_tail <= lead
            polar = norm_tail <= -lead
            safe = jnp.where(norm_tail > 0.0, norm_tail, 1.0)
            middle = 0.5 * (lead + norm_tail)
            head = jnp.where(inside, lead, jnp.where(polar, 0.0, middle))
            scale = jnp.where(inside, 1.0, jnp.where(polar, 0.0, middle / safe))
            factors = jnp.concatenate([*two_parts(head), *two_parts(scale)], axis=0)
            for i in range(PER * j, PER * j + PER):
                values = rhs_v[i] - image[i] - dual[i]
                start = jnp.broadcast_to(starts[i], (BATCH, R))
                spread = dot(factors, onehot[i])
                kept = values * (spread[64:96] + spread[96:128])
                new = jnp.where(start > 0.5, spread[0:32] + spread[32:64], kept)
                slack[i] = new
                dual[i] = dual[i] + image[i] + new - rhs_v[i]

    def turn_tech(low, high):
        def turned(i, carry):
            for b in range(0, R, 256):
                for c in range(0, 1024, 256):
                    TT[i, c : c + 256, b : b + 256] = T[i, b : b + 256, c : c + 256].T
            return carry

        lax.fori_loop(low, high, turned, 0)

    def iteration(t, carry):
        k = lax.rem(t, CG_STEPS)
        first = k == 0
        turn = lax.rem(t, 2)
        sq[...] = jnp.zeros((BATCH, 128), F32)

        def here(i):
            @pl.when(first)
            def _():
                vown[i] = (rhs_v[i] - slack[i] - dual[i] - image[i]).astype(BF16)

            @pl.when(jnp.logical_not(first))
            def _():
                vown[i] = next_image_step(i, 1 - turn).astype(BF16)

            rows_copy(i).start()

        def adjoint(mine, theirs):
            for i in theirs:
                rows_copy(i).wait_recv()

            @pl.when(t == 0)
            def _():
                for c in (*mine, *(CH + i for i in theirs)):
                    pltpu.make_async_copy(T.at[c], T.at[c], load_t.at[c]).wait()

            return sum([dot(vown[i], T[i]) for i in mine] + [dot(vpart[i], T[CH + i]) for i in theirs])

        here(0)
        here(1)
        bx[...] = adjoint((0, 1), ())
        here(2)
        bx[...] += adjoint((2,), (0, 1))
        here(3)

        @pl.when(jnp.logical_not(first))
        def _():
            curv_to_partner()

        bx[...] += adjoint((3,), (2,))

        @pl.when(jnp.logical_not(first))
        def _():
            curv_to_scens()

        total = bx[...] + adjoint((), (CH - 1,))
        for b in range(2):
            for c in range(8):
                tile = total[b * 16 : b * 16 + 16, c * 128 : c * 128 + 128]
                rs_send[b * 8 + c] = tile.astype(BF16)
        to_scens(lambda p: rs_send.at[lax.rem(p, NP)], rs_recv, 0)
        rs_recv[me] = rs_send[place]

        @pl.when(t == 0)
        def _():
            for i in range(2 * CH):
                pltpu.make_async_copy(W.at[i], W.at[i], load_w.at[i]).wait()

            def turned(i, carry):
                for b in range(0, R, 256):
                    WT[i, :, b : b + 256] = W[i, b : b + 256, :].T
                return carry

            lax.fori_loop(0, 2 * CH, turned, 0)
            turn_tech(0, CH + 1)

        for j in range(4):
            rows = vown if j < 2 else vpart
            a = PER * (j % 2)
            by[j] = sum(dot(rows[a + p], W[PER * j + p]) for p in range(PER))

        @pl.when(first)
        def _():
            alpha[...] = jnp.full((BATCH, 128), -1.0, F32)

        @pl.when(jnp.logical_not(first))
        def _():
            set_alpha()

        norm = jnp.zeros((BATCH, 128), F32)
        for j in range(4):
            r = ry[j] - wide(alpha[...], 2) * (dy[j] + by[j])
            ry[j] = r
            ly[j] = r.astype(BF16)
            norm = norm + fold(r * r)
        sq_dir[...] = norm

        all_came(rs_recv, scen_sem.at[1])
        back = jnp.sum(rs_recv[...].astype(F32), axis=0)
        res = rx[...] - alpha[rows16, :] * (dx[...] + back)
        rx[...] = res
        ag[place] = res.astype(BF16)
        to_plane(ag, 4)
        sq_dir[rows16, :] += 0.5 * (res * res)
        norm_all[me] = to_row(sq_dir[...])
        to_scens(lambda p: norm_all.at[me], norm_all, 6)
        add_steps()
        all_came(rs_recv, scen_sem.at[0])
        for i in range(CH):
            rows_copy(i).wait_send()
        for i in range(CH):
            pps[i] = dot(ly[2 + i // PER], WT[CH + i])
            own[i] = dot(ly[i // PER], WT[i])

        @pl.when(t == 0)
        def _():
            turn_tech(CH + 1, 2 * CH)

        all_came(ag, scen_sem.at[5])
        for b in range(2):
            for c in range(8):
                lx[b * 16 : b * 16 + 16, c * 128 : c * 128 + 128] = ag[b * 8 + c]

        def exchange(i):
            partial_copy(i).wait_recv()
            here = own[i] + ppr[i]
            own[i] = here
            zs[i] = here.astype(BF16)
            across_copy(i, turn).start()

        def for_partner(i):
            pps[i] += dot(lx[...], TT[CH + i])
            partial_copy(i).start()

        def for_here(i):
            own[i] += dot(lx[...], TT[i])

        for_partner(0)
        for_here(0)
        for_partner(1)
        exchange(0)
        for_partner(2)
        for_here(1)
        exchange(1)
        all_came(norm_all, scen_sem.at[7])
        norm_col[col] = jnp.sum(norm_all[...], axis=0)
        to_cols(norm_col, 2)
        for_partner(3)
        for_here(2)
        exchange(2)
        for_here(3)
        exchange(3)

        all_came(norm_all, scen_sem.at[6])
        all_came(ag, scen_sem.at[4])
        all_came(norm_col, col_sem.at[3])
        all_came(norm_col, col_sem.at[2])
        new_norm = jnp.sum(norm_col[...], axis=0)

        @pl.when(first)
        def _():
            beta[...] = jnp.zeros((BATCH, 128), F32)
            for i in range(CH):
                q[i] = jnp.zeros((BATCH, R), F32)

        @pl.when(jnp.logical_not(first))
        def _():
            beta[...] = to_columns(new_norm / nres[...])

        nres[...] = new_norm
        norm = jnp.zeros((BATCH, 128), F32)
        for j in range(4):
            d = ry[j] + wide(beta[...], 2) * dy[j]
            dy[j] = d
            norm = norm + fold(d * d)
        sq_dir[...] = norm
        d = rx[...] + beta[rows16, :] * dx[...]
        dx[...] = d
        sq_dir[rows16, :] += 0.5 * (d * d)
        dir_col[col] = to_row(sq_dir[...])
        to_cols(dir_col, 0)
        for i in range(CH):
            partial_copy(i).wait_send()

        @pl.when(k == CG_STEPS - 1)
        def _():
            sq[...] = jnp.zeros((BATCH, 128), F32)
            for i in range(CH):
                next_image_step(i, turn)
            curv_to_partner()
            curv_to_scens()
            set_alpha()
            add_steps()

            @pl.when(t == ITERS * CG_STEPS - 1)
            def _():
                xg[place] = x[...]
                to_plane(xg, 8)

            set_costs()
            for i in range(CH):
                q[i] = jnp.zeros((BATCH, R), F32)
            project()

        return carry

    lax.fori_loop(0, ITERS * CG_STEPS, iteration, 0)

    if PER == 2:
        here = there = col // 2
        lanes_here = pl.ds(pl.multiple_of(core * 512, 128), 512)
        lanes_there = pl.ds(pl.multiple_of((1 - core) * 512, 128), 512)
    else:
        here, there = col, partner
        lanes_here = lanes_there = slice(None)

    def last_copy(a, j):
        return pltpu.make_async_remote_copy(
            (slack, dual)[a].at[PER * j + there, :, lanes_there], fin.at[a, j],
            fin_sem.at[0, a, j], fin_sem.at[1, a, j],
            device_id={"col": partner}, device_id_type=MESH,
        )

    for a in range(2):
        for j in range(2):
            last_copy(a, j).start()
    for j in range(2):
        slack_out[core * 2 + j] = slack[PER * j + here, :, lanes_here]
        dual_out[core * 2 + j] = dual[PER * j + here, :, lanes_here]
        second_out[core * 2 + j] = y[j]
        second_out[(1 - core) * 2 + j] = y[2 + j]
    for a in range(2):
        for j in range(2):
            last_copy(a, j).wait()
            (slack_out, dual_out)[a][(1 - core) * 2 + j] = fin[a, j]
    all_came(xg, scen_sem.at[9])
    all_came(xg, scen_sem.at[8])
    for b in range(2):
        for c in range(8):
            first_out[b * 16 : b * 16 + 16, c * 128 : c * 128 + 128] = xg[b * 8 + c]


def finish(first, second, slack, dual, first_out, second_out, slack_out, dual_out):
    first_out[...] = first[...]
    for j in range(4):
        second_out[:, j, :] = second[j]
        slack_out[:, j, :] = slack[j]
        dual_out[:, j, :] = dual[j]


def body(tech, recourse, rhs, cost_first, cost_second, cone_id):
    any_space = pl.BlockSpec(memory_space=pl.ANY)
    vmem = pl.BlockSpec(memory_space=pltpu.VMEM)
    rows_f32 = pltpu.VMEM((CH, BATCH, R), F32)
    rows_bf16 = pltpu.VMEM((CH, BATCH, R), BF16)
    block = pltpu.VMEM((16, 128), F32)
    ys = pltpu.VMEM((4, BATCH, 256), F32)
    dma = pltpu.SemaphoreType.DMA
    first, second, slack, dual = pl.pallas_call(
        kernel,
        out_shape=(
            jax.ShapeDtypeStruct((BATCH, 1024), F32),
            jax.ShapeDtypeStruct((4, BATCH, 256), F32),
            jax.ShapeDtypeStruct((4, BATCH, 512), F32),
            jax.ShapeDtypeStruct((4, BATCH, 512), F32),
        ),
        in_specs=[any_space, any_space, any_space, vmem, vmem, vmem],
        out_specs=(vmem, vmem, vmem, vmem),
        scratch_shapes=[
            pltpu.VMEM((2 * CH, R, 1024), BF16),
            pltpu.VMEM((2 * CH, R, 256), BF16),
            pltpu.VMEM((2 * CH, 1024, R), BF16),
            pltpu.VMEM((2 * CH, 256, R), BF16),
            rows_f32, rows_f32, rows_f32, rows_f32, rows_f32,
            rows_f32, rows_f32, rows_f32,
            rows_bf16, pltpu.VMEM((2, CH, BATCH, R), BF16),
            rows_bf16, rows_bf16,
            pltpu.VMEM((BATCH, 1024), F32),
            pltpu.VMEM((BATCH, 1024), BF16),
            pltpu.VMEM((CH, NCONE, R), BF16),
            pltpu.VMEM((CH, 1, R), F32),
            block, block, block,
            ys, ys, ys, ys,
            pltpu.VMEM((4, BATCH, 256), BF16),
            pltpu.VMEM((NP, 16, 128), BF16),
            pltpu.VMEM((NS, 16, 128), BF16),
            pltpu.VMEM((NP, 16, 128), BF16),
            pltpu.VMEM((NP, 16, 128), F32),
            pltpu.VMEM((NS, 1, 128), F32),
            pltpu.VMEM((NS, 1, 128), F32),
            pltpu.VMEM((2, 1, 128), F32),
            pltpu.VMEM((NC, 1, 128), F32),
            pltpu.VMEM((NC, 1, 128), F32),
            pltpu.VMEM((1, 128), F32),
            pltpu.VMEM((BATCH, 128), F32),
            pltpu.VMEM((BATCH, 128), F32),
            pltpu.VMEM((BATCH, 128), F32),
            pltpu.VMEM((BATCH, 128), F32),
            pltpu.VMEM((2, 2, BATCH, 512), F32),
            dma((2 * CH,)), dma((2 * CH,)), dma((CH,)),
            dma((2, CH)), dma((2, CH)), dma((3, CH)),
            dma((10,)), dma((4,)), dma((2,)), dma((2, 2, 2)),
        ],
        compiler_params=pltpu.CompilerParams(
            collective_id=0, has_side_effects=True, vmem_limit_bytes=60 * 2**20
        ),
    )(
        tech,
        recourse,
        rhs,
        cost_first.reshape(8, 1, 128),
        cost_second,
        cone_id,
    )
    return pl.pallas_call(
        finish,
        out_shape=(
            jax.ShapeDtypeStruct((BATCH, 1024), F32),
            jax.ShapeDtypeStruct((BATCH, 4, 256), F32),
            jax.ShapeDtypeStruct((BATCH, 4, 512), F32),
            jax.ShapeDtypeStruct((BATCH, 4, 512), F32),
        ),
        in_specs=[vmem, vmem, vmem, vmem],
        out_specs=(vmem, vmem, vmem, vmem),
    )(first, second, slack, dual)


def solution(mesh):
    return jax.shard_map(
        body,
        mesh=mesh,
        in_specs=(
            P("scen", None, "col"),
            P("scen", None, "col"),
            P(None, "scen", None),
            P("col"),
            P("scen", "col"),
            P("scen", None),
        ),
        out_specs=(
            P(None, "col"),
            P(None, "scen", "col"),
            P(None, "scen", "col"),
            P(None, "scen", "col"),
        ),
        check_vma=False,
    )
```
